32 devices in a mesh: dp: 4 (over y, x), mp: 8 (over z, core).
Axes of the slice: x: 2, y: 2, z: 4, core: 2. Of those that a mesh axis runs over, the one named last changes fastest.
Arguments:
- rewards: int32 [32], P('dp'), may hold values from 0 to 4096, as said below
- group_ids: int32 [32], P('dp'), may hold values from 0 to 1, as said below
- lengths: int32 [32], P('dp'), may hold values from 1 to 64
- token_mask: int32 [2048], P('dp'), may hold values from 0 to 1, as said below
- targets: int32 [2048], P('dp'), may hold values from 0 to 65535
- logits: bfloat16 [2048, 65536], P('dp', 'mp'), may hold values from -140 to 400
Outputs:
- advantage: float32 [32], P('dp')
- token_weight: float32 [2048], P('dp')
- token_logprob: float32 [2048], P('dp')
- token_entropy: float32 [2048], P('dp')
- objective: float32 [], replicated
The draws below stay inside these ranges and needn't reach their ends.
Inputs may be any that keep to these rules, and one draw needn't show every extreme that they name: rewards in units of 1/1024. `group_ids`: each of the 2 prompts has exactly 16 trajectories. `token_mask`: zeros come in aligned spans of 8 positions, except that the first position of each window is always 1.
All inputs are finite; a program needn't handle non-finite values.
Results may differ from the reference program's by a relative error of at most 0.00095.
Values may be sent and summed in bfloat16 or wider, within the bound.
A program may use at most 64 MiB of HBM per device.

```python
import math
import jax
import jax.numpy as jnp
from jax import lax

VOCAB = 65536
GROUP = 16
WIN = 64
ROLLOUTS = 32
GROUPS = 2
TOKENS = 2048


def group_plan(key):
    shuffled = jax.random.permutation(jax.random.fold_in(key, 11), ROLLOUTS)
    return (shuffled // GROUP).astype(jnp.int32)


def draw_group_ids(key, part):
    return group_plan(key)


def draw_rewards(key, part):
    groups_of = group_plan(key)
    own_values = jax.random.randint(jax.random.fold_in(key, 12), (ROLLOUTS,), 0, 4097)
    shared_value = jax.random.randint(jax.random.fold_in(key, 13), (GROUPS,), 0, 4097)
    flat_group = jax.random.randint(jax.random.fold_in(key, 14), (GROUPS,), 0, 2)
    flat_group = flat_group * (jnp.arange(GROUPS, dtype=jnp.int32) > 0)
    return jnp.where(flat_group[groups_of] > 0, shared_value[groups_of], own_values).astype(jnp.int32)


def draw_lengths(key, part):
    rollout_index = jnp.arange(ROLLOUTS, dtype=jnp.int32)
    upper_bound = WIN // 3 + (WIN - WIN // 3) * rollout_index // max(ROLLOUTS - 1, 1)
    drawn_lengths = jax.random.randint(jax.random.fold_in(key, 21), (ROLLOUTS,), 1, upper_bound + 1)
    return jnp.where(rollout_index == ROLLOUTS - 1, WIN, drawn_lengths).astype(jnp.int32)


def draw_token_mask(key, part):
    span_bits = jax.random.randint(jax.random.fold_in(key, 31), (TOKENS // 8,), 0, 4)
    span_live = jnp.repeat(span_bits > 0, 8)
    opening = jnp.arange(TOKENS, dtype=jnp.int32) % WIN == 0
    return jnp.where(opening | span_live, 1, 0).astype(jnp.int32)


def target_plan(key):
    return jax.random.randint(jax.random.fold_in(key, 51), (TOKENS,), 0, VOCAB).astype(jnp.int32)


def draw_targets(key, part):
    return target_plan(key)


def draw_logits(key, part):
    row_scale = jnp.exp(jax.random.uniform(jax.random.fold_in(key, 61), (TOKENS, 1), jnp.float32, 0.0, math.log(10.0)))
    column_scale = jnp.exp(jax.random.uniform(jax.random.fold_in(key, 62), (1, VOCAB), jnp.float32, 0.0, math.log(10.0)))
    normal_part = jnp.clip(jax.random.normal(jax.random.fold_in(key, 63), (TOKENS, VOCAB), jnp.float32), -4.5, 4.5)
    base_logits = 0.3 * normal_part * row_scale * column_scale
    target_lift = jax.random.uniform(jax.random.fold_in(key, 65), (TOKENS, 1), jnp.float32, -3.0, 1.0)
    chosen = jnp.arange(VOCAB, dtype=jnp.int32)[None, :] == target_plan(key)[:, None]
    planted = jnp.where(chosen, jnp.max(base_logits, axis=1, keepdims=True) + target_lift, base_logits)
    return planted.astype(jnp.bfloat16)


def setup_inputs(seed: int = 0) -> dict:
    seeds = jax.random.split(jax.random.key(seed), 7)
    return {
        "rewards": draw_rewards(jax.random.fold_in(seeds[6], 71), 0),
        "group_ids": draw_group_ids(jax.random.fold_in(seeds[6], 71), 0),
        "lengths": draw_lengths(jax.random.fold_in(seeds[6], 71), 0),
        "token_mask": draw_token_mask(jax.random.fold_in(seeds[6], 71), 0),
        "targets": draw_targets(jax.random.fold_in(seeds[6], 71), 0),
        "logits": draw_logits(jax.random.fold_in(seeds[6], 71), 0),
    }


spread_floor = 0.25
reward_unit = 1024.0
highest = lax.Precision.HIGHEST

def window_statistics(inputs):
    logit_rows, row_targets = inputs
    values = logit_rows.astype(jnp.float32)
    row_peak = lax.optimization_barrier(jnp.max(values, axis=1))
    shifted = values - row_peak[:, None]
    weights = jnp.exp(shifted)
    totals = lax.optimization_barrier(jnp.sum(weights, axis=1))
    log_total = row_peak + jnp.log(totals)
    picked = jnp.take_along_axis(values, row_targets[:, None].astype(jnp.int32), axis=1)[:, 0]
    entropy = jnp.log(totals) - lax.optimization_barrier(jnp.sum(weights * shifted, axis=1)) / totals
    return (picked - log_total, entropy)

def reference(rewards, group_ids, lengths, token_mask, targets, logits):
    log_prob, entropy = lax.map(window_statistics, (logits.reshape(ROLLOUTS, WIN, VOCAB), targets.reshape(ROLLOUTS, WIN)))
    positions = jnp.arange(WIN, dtype=jnp.int32)
    live_mask = ((token_mask.reshape(ROLLOUTS, WIN) > 0) & (positions[None, :] < lengths[:, None])).astype(jnp.float32)
    token_logprob = live_mask * log_prob
    token_entropy = live_mask * entropy
    counts = lax.optimization_barrier(jnp.sum(live_mask, axis=1))
    reward_values = rewards.astype(jnp.float32) / reward_unit
    member = (group_ids[:, None] == jnp.arange(GROUPS, dtype=jnp.int32)[None, :]).astype(jnp.float32)
    group_mean = jnp.dot(reward_values, member, precision=highest) / GROUP
    centred = reward_values - jnp.dot(member, group_mean, precision=highest)
    group_var = jnp.dot(centred * centred, member, precision=highest) / GROUP
    group_spread = jnp.maximum(jnp.sqrt(group_var), spread_floor)
    group_tokens = jnp.dot(counts, member, precision=highest)
    advantage = centred / jnp.dot(member, group_spread, precision=highest)
    token_scale = GROUP * WIN / jnp.dot(member, group_tokens, precision=highest)
    token_weight = live_mask * (advantage * token_scale)[:, None]
    objective = -jnp.sum(token_weight * token_logprob) / (ROLLOUTS * WIN)
    return (advantage, token_weight.reshape(-1), token_logprob.reshape(-1), token_entropy.reshape(-1), objective)
```

```python
import functools

import jax
import jax.numpy as jnp
from jax import lax
from jax.experimental import pallas as pl
from jax.experimental.pallas import tpu as pltpu
from jax.sharding import PartitionSpec as P

GROUP = 16
WIN = 64
LANES = 128
STEP = 16
CHUNKS = 8

spread_floor = 0.25
reward_unit = 1024.0
MESH = pl.DeviceIdType.MESH


def each(first, last, visit):
    if last - first <= 16:
        for k in range(first, last):
            visit(k)
    else:
        lax.fori_loop(first, last, lambda k, carry: (visit(k), carry)[1], 0)


def kernel(
    dp_size,
    mp_size,
    rewards_s,
    groups_s,
    lengths_s,
    rewards_v,
    groups_v,
    mask_v,
    targets_v,
    logits_hbm,
    advantage_out,
    weight_out,
    logprob_out,
    entropy_out,
    objective_out,
    *scratch,
):
    chunks = scratch[:CHUNKS]
    (
        peak_rows,
        total_rows_ref,
        moment_rows,
        target_rows,
        columns,
        stats,
        gathered,
        facts,
        facts_all,
        part,
        parts,
        load_sem,
        stat_send,
        stat_recv,
        fact_send,
        fact_recv,
        part_send,
        part_recv,
    ) = scratch[CHUNKS:]
    rows, vocab = logits_hbm.shape
    rollouts = rewards_v.shape[1]
    bands = rows // LANES
    groups = rollouts * dp_size // GROUP
    chunk_rows = rows // CHUNKS
    tiles = vocab // LANES
    me_dp = lax.axis_index("dp")
    me_mp = lax.axis_index("mp")
    f32 = jnp.float32

    loads = [
        pltpu.make_async_copy(
            logits_hbm.at[pl.ds(c * chunk_rows, chunk_rows), :], chunks[c], load_sem.at[c]
        )
        for c in range(CHUNKS)
    ]
    for load in loads:
        load.start()

    barrier = pltpu.get_barrier_semaphore()

    def greet_mp(k):
        peer = lax.rem(me_mp + k, mp_size)
        pl.semaphore_signal(barrier, inc=1, device_id=(me_dp, peer), device_id_type=MESH)

    def greet_dp(k):
        peer = lax.rem(me_dp + k, dp_size)
        pl.semaphore_signal(barrier, inc=1, device_id=(peer, me_mp), device_id_type=MESH)

    each(1, mp_size, greet_mp)
    each(1, dp_size, greet_dp)

    lane = lax.broadcasted_iota(jnp.int32, (bands, LANES), 1)
    band = lax.broadcasted_iota(jnp.int32, (bands, LANES), 0)
    owner = band * (LANES // WIN) + lane // WIN
    position = lax.rem(lane, WIN)
    reward_tok = jnp.zeros((bands, LANES), jnp.int32)
    group_tok = jnp.zeros((bands, LANES), jnp.int32)
    length_tok = jnp.zeros((bands, LANES), jnp.int32)
    for k in range(rollouts):
        here = owner == k
        reward_tok = jnp.where(here, rewards_s[k], reward_tok)
        group_tok = jnp.where(here, groups_s[k], group_tok)
        length_tok = jnp.where(here, lengths_s[k], length_tok)
    live = jnp.where((mask_v[...] > 0) & (position < length_tok), 1.0, 0.0).astype(f32)
    reward_tok = reward_tok.astype(f32) / reward_unit
    facts[0:bands, :] = reward_tok
    facts[bands : 2 * bands, :] = group_tok.astype(f32)
    facts[2 * bands : 3 * bands, :] = live

    base = me_mp * vocab
    for b in range(bands):
        spread_out = jnp.broadcast_to(targets_v[b : b + 1, :], (LANES, LANES))
        columns[b * LANES : (b + 1) * LANES, :] = spread_out.T

    for c in range(CHUNKS):
        loads[c].wait()
        chunk = chunks[c]

        def step(i, carry, c=c, chunk=chunk):
            start = pl.multiple_of(i * STEP, STEP)
            where_out = pl.ds(pl.multiple_of(c * chunk_rows + i * STEP, STEP), STEP)
            span = pl.ds(start, STEP)
            column = lax.shift_right_arithmetic(columns[where_out, :] - base, 7)
            bits = [
                jnp.bitwise_and(lax.shift_right_arithmetic(column, k), 1).astype(f32)
                for k in range(max(tiles - 1, 0).bit_length())
            ]
            bits = [bit.astype(jnp.bfloat16) > 0.5 for bit in bits]

            def survey(first, size):
                if size == 1:
                    tile = chunk[span, first * LANES : (first + 1) * LANES]
                    return tile, tile
                half = size // 2
                low = survey(first, half)
                if first + half >= tiles:
                    return low
                top = survey(first + half, half)
                chosen = jnp.where(bits[half.bit_length() - 1], top[1], low[1])
                return jnp.maximum(low[0], top[0]), chosen

            high, held = survey(0, 1 << max(tiles - 1, 0).bit_length())
            target_rows[where_out, :] = held.astype(f32)
            high = high.astype(f32)
            total = jnp.zeros((STEP, LANES), f32)
            moment = jnp.zeros((STEP, LANES), f32)
            for j in range(tiles):
                shifted = chunk[span, j * LANES : (j + 1) * LANES].astype(f32) - high
                weight = jnp.exp(shifted)
                total += weight
                moment += weight * shifted
            peak_rows[where_out, :] = high
            total_rows_ref[where_out, :] = total
            moment_rows[where_out, :] = moment
            return carry

        lax.fori_loop(0, chunk_rows // STEP, step, 0)

        if c == 0:
            pl.semaphore_wait(barrier, mp_size + dp_size - 2)

            def send_fact(k):
                peer = lax.rem(me_dp + k, dp_size)
                pltpu.make_async_remote_copy(
                    src_ref=facts,
                    dst_ref=facts_all.at[me_dp],
                    send_sem=fact_send.at[k],
                    recv_sem=fact_recv.at[me_dp],
                    device_id=(peer, me_mp),
                    device_id_type=MESH,
                ).start()

            each(1, dp_size, send_fact)

    sub = lax.broadcasted_iota(jnp.int32, (LANES, LANES), 0)
    for b in range(bands):
        block = slice(b * LANES, (b + 1) * LANES)
        high = peak_rows[block, :].T
        total = total_rows_ref[block, :].T
        moment = moment_rows[block, :].T
        held = target_rows[block, :].T
        peak = jnp.max(high, axis=0, keepdims=True)
        gap = high - peak
        factor = jnp.exp(gap)
        local = targets_v[b : b + 1, :] - base
        inside = (local >= 0) & (local < vocab)
        at_lane = jnp.where(inside, jnp.bitwise_and(local, LANES - 1), -1)
        stats[b : b + 1, :] = peak
        stats[bands + b : bands + b + 1, :] = jnp.sum(factor * total, axis=0, keepdims=True)
        stats[2 * bands + b : 2 * bands + b + 1, :] = jnp.sum(
            factor * (moment + gap * total), axis=0, keepdims=True
        )
        stats[3 * bands + b : 3 * bands + b + 1, :] = jnp.sum(
            jnp.where(sub == at_lane, held, 0.0), axis=0, keepdims=True
        )

    def stat_copy(k, slot):
        peer = lax.rem(me_mp + k, mp_size)
        return pltpu.make_async_remote_copy(
            src_ref=stats,
            dst_ref=gathered.at[slot],
            send_sem=stat_send.at[k],
            recv_sem=stat_recv.at[slot],
            device_id=(me_dp, peer),
            device_id_type=MESH,
        )

    each(1, mp_size, lambda k: stat_copy(k, me_mp).start())
    gathered[me_mp] = stats[...]

    def fact_copy(k, slot):
        peer = lax.rem(me_dp + k, dp_size)
        return pltpu.make_async_remote_copy(
            src_ref=facts,
            dst_ref=facts_all.at[slot],
            send_sem=fact_send.at[k],
            recv_sem=fact_recv.at[slot],
            device_id=(peer, me_mp),
            device_id_type=MESH,
        )

    facts_all[me_dp] = facts[...]
    each(1, dp_size, lambda k: fact_copy(k, lax.rem(me_dp + dp_size - k, dp_size)).wait_recv())
    all_reward = facts_all[:, 0:bands, :]
    all_group = facts_all[:, bands : 2 * bands, :]
    all_live = facts_all[:, 2 * bands : 3 * bands, :]

    def whole_sum(values):
        flat = jnp.sum(values, axis=0)
        return jnp.sum(jnp.sum(flat, axis=1, keepdims=True), axis=0, keepdims=True)

    reward_row = rewards_v[...].astype(f32) / reward_unit
    mean_row = jnp.zeros((1, rollouts), f32)
    spread_row = jnp.ones((1, rollouts), f32)
    mean_tok = jnp.zeros((bands, LANES), f32)
    spread_tok = jnp.ones((bands, LANES), f32)
    scale_tok = jnp.zeros((bands, LANES), f32)
    for g in range(groups):
        member = jnp.where(all_group == float(g), 1.0, 0.0).astype(f32)
        mean = whole_sum(member * all_reward) / (GROUP * WIN)
        apart = all_reward - mean[None]
        variance = whole_sum(member * apart * apart) / (GROUP * WIN)
        spread = jnp.maximum(jnp.sqrt(variance), spread_floor)
        scale = (GROUP * WIN) / whole_sum(member * all_live)
        in_row = groups_v[...] == g
        in_tok = group_tok == g
        mean_row = jnp.where(in_row, mean, mean_row)
        spread_row = jnp.where(in_row, spread, spread_row)
        mean_tok = jnp.where(in_tok, mean, mean_tok)
        spread_tok = jnp.where(in_tok, spread, spread_tok)
        scale_tok = jnp.where(in_tok, scale, scale_tok)
    advantage_out[...] = (reward_row - mean_row) / spread_row
    weight = live * ((reward_tok - mean_tok) / spread_tok * scale_tok)
    weight_out[...] = weight

    each(1, mp_size, lambda k: stat_copy(k, lax.rem(me_mp + mp_size - k, mp_size)).wait_recv())
    peaks = gathered[:, 0:bands, :]
    peak = jnp.max(peaks, axis=0)
    gap = peaks - peak[None]
    factor = jnp.exp(gap)
    totals = gathered[:, bands : 2 * bands, :]
    total = jnp.sum(factor * totals, axis=0)
    moment = jnp.sum(factor * (gathered[:, 2 * bands : 3 * bands, :] + gap * totals), axis=0)
    target = jnp.sum(gathered[:, 3 * bands : 4 * bands, :], axis=0)
    log_total = jnp.log(total)
    logprob = live * (target - (peak + log_total))
    logprob_out[...] = logprob
    own = jnp.sum(jnp.sum(weight * logprob, axis=1, keepdims=True), axis=0, keepdims=True)
    part[...] = jnp.broadcast_to(own, part.shape)

    def part_copy(k, slot):
        peer = lax.rem(me_dp + k, dp_size)
        return pltpu.make_async_remote_copy(
            src_ref=part,
            dst_ref=parts.at[slot],
            send_sem=part_send.at[k],
            recv_sem=part_recv.at[slot],
            device_id=(peer, me_mp),
            device_id_type=MESH,
        )

    each(1, dp_size, lambda k: part_copy(k, me_dp).start())
    parts[me_dp] = part[...]
    entropy_out[...] = live * (log_total - moment / total)

    each(1, dp_size, lambda k: fact_copy(k, me_dp).wait_send())
    each(1, mp_size, lambda k: stat_copy(k, me_mp).wait_send())
    each(1, dp_size, lambda k: part_copy(k, lax.rem(me_dp + dp_size - k, dp_size)).wait_recv())
    summed = jnp.sum(parts[...], axis=0)[0:1, 0:1]
    objective_out[...] = -summed / (groups * GROUP * WIN)
    each(1, dp_size, lambda k: part_copy(k, me_dp).wait_send())


def hand_over(*refs):
    half = len(refs) // 2
    for source, result in zip(refs[:half], refs[half:]):
        result[...] = source[...]


def shards(dp_size, mp_size, rewards, group_ids, lengths, token_mask, targets, logits):
    rows, vocab = logits.shape
    rollouts = lengths.shape[0]
    bands = rows // LANES
    f32 = jnp.float32
    smem = pl.BlockSpec(memory_space=pltpu.SMEM)
    vmem = pl.BlockSpec(memory_space=pltpu.VMEM)
    outs = pl.pallas_call(
        functools.partial(kernel, dp_size, mp_size),
        out_shape=(
            jax.ShapeDtypeStruct((1, rollouts), f32),
            jax.ShapeDtypeStruct((bands, LANES), f32),
            jax.ShapeDtypeStruct((bands, LANES), f32),
            jax.ShapeDtypeStruct((bands, LANES), f32),
            jax.ShapeDtypeStruct((1, 1), f32),
        ),
        in_specs=[smem] * 3 + [vmem] * 4 + [pl.BlockSpec(memory_space=pl.ANY)],
        out_specs=(vmem,) * 5,
        scratch_shapes=[pltpu.VMEM((rows // CHUNKS, vocab), logits.dtype)] * CHUNKS
        + [pltpu.VMEM((rows, LANES), f32)] * 4
        + [pltpu.VMEM((rows, LANES), jnp.int32)]
        + [
            pltpu.VMEM((4 * bands, LANES), f32),
            pltpu.VMEM((mp_size, 4 * bands, LANES), f32),
            pltpu.VMEM((3 * bands, LANES), f32),
            pltpu.VMEM((dp_size, 3 * bands, LANES), f32),
            pltpu.VMEM((8, LANES), f32),
            pltpu.VMEM((dp_size, 8, LANES), f32),
            pltpu.SemaphoreType.DMA((CHUNKS,)),
            pltpu.SemaphoreType.DMA((mp_size,)),
            pltpu.SemaphoreType.DMA((mp_size,)),
            pltpu.SemaphoreType.DMA((dp_size,)),
            pltpu.SemaphoreType.DMA((dp_size,)),
            pltpu.SemaphoreType.DMA((dp_size,)),
            pltpu.SemaphoreType.DMA((dp_size,)),
        ],
        compiler_params=pltpu.CompilerParams(collective_id=0, has_side_effects=True),
    )(
        rewards,
        group_ids,
        lengths,
        rewards.reshape(1, rollouts),
        group_ids.reshape(1, rollouts),
        token_mask.reshape(bands, LANES),
        targets.reshape(bands, LANES),
        logits,
    )
    outs = pl.pallas_call(
        hand_over,
        out_shape=[jax.ShapeDtypeStruct(value.shape, value.dtype) for value in outs],
        in_specs=[vmem] * 5,
        out_specs=[vmem] * 5,
    )(*outs)
    advantage, weight, logprob, entropy, objective = outs
    return (
        advantage.reshape(-1),
        weight.reshape(-1),
        logprob.reshape(-1),
        entropy.reshape(-1),
        objective.reshape(()),
    )


def solution(mesh):
    in_specs = (P("dp"), P("dp"), P("dp"), P("dp"), P("dp"), P("dp", "mp"))
    out_specs = (P("dp"), P("dp"), P("dp"), P("dp"), P())
    body = functools.partial(shards, mesh.shape["dp"], mesh.shape["mp"])
    return jax.shard_map(body, mesh=mesh, in_specs=in_specs, out_specs=out_specs, check_vma=False)
```

```python
import functools

import jax
import jax.numpy as jnp
from jax import lax
from jax.experimental import pallas as pl
from jax.experimental.pallas import tpu as pltpu
from jax.sharding import PartitionSpec as P

GROUP = 16
WIN = 64
LANES = 128
STEP = 16
CHUNKS = 8
SUM_ROWS = 16
SUM_TILES = 64
PARTS = 4

spread_floor = 0.25
reward_unit = 1024.0
MESH = pl.DeviceIdType.MESH


def each(first, last, visit):
    if last - first <= 16:
        for k in range(first, last):
            visit(k)
    else:
        lax.fori_loop(first, last, lambda k, carry: (visit(k), carry)[1], 0)


def kernel(
    dp_size,
    mp_size,
    rewards_hbm,
    groups_hbm,
    lengths_hbm,
    rewards_row_hbm,
    groups_row_hbm,
    mask_hbm,
    targets_hbm,
    logits_hbm,
    result,
    block_rows,
    rewards_s,
    groups_s,
    lengths_s,
    rewards_v,
    groups_v,
    mask_v,
    targets_v,
    peak_rows,
    total_rows_ref,
    moment_rows,
    target_rows,
    columns,
    stats,
    gathered,
    facts,
    facts_all,
    part,
    parts,
    load_sem,
    small_sem,
    stat_send,
    stat_recv,
    fact_send,
    fact_recv,
    part_send,
    part_recv,
):
    rows, vocab = logits_hbm.shape
    rollouts = rewards_v.shape[1]
    bands = rows // LANES
    groups = rollouts * dp_size // GROUP
    tiles = vocab // LANES
    me_dp = lax.axis_index("dp")
    me_mp = lax.axis_index("mp")
    f32 = jnp.float32

    def load(i):
        span = pl.ds(pl.multiple_of(i * STEP, STEP), STEP)
        return pltpu.make_async_copy(logits_hbm.at[span, :], block_rows.at[span, :], load_sem.at[i])

    steps = rows // STEP
    for i in range(steps):
        load(i).start()
    small = [
        pltpu.make_async_copy(source, target, small_sem.at[k])
        for k, (source, target) in enumerate(
            (
                (rewards_hbm, rewards_s),
                (groups_hbm, groups_s),
                (lengths_hbm, lengths_s),
                (rewards_row_hbm, rewards_v),
                (groups_row_hbm, groups_v),
                (mask_hbm, mask_v),
                (targets_hbm, targets_v),
            )
        )
    ]
    for copy in small:
        copy.start()

    barrier = pltpu.get_barrier_semaphore()

    def greet_mp(k):
        peer = lax.rem(me_mp + k, mp_size)
        pl.semaphore_signal(barrier, inc=1, device_id=(me_dp, peer), device_id_type=MESH)

    def greet_dp(k):
        peer = lax.rem(me_dp + k, dp_size)
        pl.semaphore_signal(barrier, inc=1, device_id=(peer, me_mp), device_id_type=MESH)

    each(1, mp_size, greet_mp)
    each(1, dp_size, greet_dp)

    for copy in small:
        copy.wait()

    lane = lax.broadcasted_iota(jnp.int32, (bands, LANES), 1)
    band = lax.broadcasted_iota(jnp.int32, (bands, LANES), 0)
    owner = band * (LANES // WIN) + lane // WIN
    position = lax.rem(lane, WIN)
    reward_tok = jnp.zeros((bands, LANES), jnp.int32)
    group_tok = jnp.zeros((bands, LANES), jnp.int32)
    length_tok = jnp.zeros((bands, LANES), jnp.int32)
    for k in range(rollouts):
        here = owner == k
        reward_tok = jnp.where(here, rewards_s[k], reward_tok)
        group_tok = jnp.where(here, groups_s[k], group_tok)
        length_tok = jnp.where(here, lengths_s[k], length_tok)
    live = jnp.where((mask_v[...] > 0) & (position < length_tok), 1.0, 0.0).astype(f32)
    reward_tok = reward_tok.astype(f32) / reward_unit
    facts[0:bands, :] = reward_tok
    facts[bands : 2 * bands, :] = group_tok.astype(f32)
    facts[2 * bands : 3 * bands, :] = live

    base = me_mp * vocab
    for b in range(bands):
        spread_out = jnp.broadcast_to(targets_v[b : b + 1, :], (LANES, LANES))
        columns[b * LANES : (b + 1) * LANES, :] = spread_out.T

    levels = max(tiles - 1, 0).bit_length()

    def survey_step(i, carry):
        load(i).wait()
        span = pl.ds(pl.multiple_of(i * STEP, STEP), STEP)
        column = lax.shift_right_arithmetic(columns[span, :] - base, 7)
        bits = [
            jnp.bitwise_and(lax.shift_right_arithmetic(column, k), 1).astype(f32)
            for k in range(levels)
        ]
        bits = [bit.astype(jnp.bfloat16) > 0.5 for bit in bits]

        def survey(first, size):
            if size == 1:
                tile = block_rows[span, first * LANES : (first + 1) * LANES]
                return tile, tile
            half = size // 2
            low = survey(first, half)
            if first + half >= tiles:
                return low
            top = survey(first + half, half)
            chosen = jnp.where(bits[half.bit_length() - 1], top[1], low[1])
            return jnp.maximum(low[0], top[0]), chosen

        high, held = survey(0, 1 << levels)
        target_rows[span, :] = held.astype(f32)
        peak_rows[span, :] = high.astype(f32)
        return carry

    block = min(SUM_TILES, tiles)

    def sum_step(i, carry):
        span = pl.ds(pl.multiple_of(i * SUM_ROWS, SUM_ROWS), SUM_ROWS)
        high = peak_rows[span, :]

        def add_block(q, sums):
            totals, moments = list(sums[:PARTS]), list(sums[PARTS:])
            for j in range(block):
                at = pl.ds(pl.multiple_of((q * block + j) * LANES, LANES), LANES)
                shifted = block_rows[span, at].astype(f32) - high
                weight = jnp.exp(shifted)
                totals[j % PARTS] += weight
                moments[j % PARTS] += weight * shifted
            return (*totals, *moments)

        zero = jnp.zeros((SUM_ROWS, LANES), f32)
        sums = lax.fori_loop(0, tiles // block, add_block, (zero,) * (2 * PARTS))
        total_rows_ref[span, :] = functools.reduce(jnp.add, sums[:PARTS])
        moment_rows[span, :] = functools.reduce(jnp.add, sums[PARTS:])
        return carry

    def chunk_step(c, carry):
        first = c * (steps // CHUNKS)
        lax.fori_loop(first, first + steps // CHUNKS, survey_step, 0)
        low = c * (rows // SUM_ROWS // CHUNKS)
        lax.fori_loop(low, low + rows // SUM_ROWS // CHUNKS, sum_step, 0)
        return carry

    split = CHUNKS - 2
    lax.fori_loop(0, split, chunk_step, 0)
    pl.semaphore_wait(barrier, mp_size + dp_size - 2)

    def fact_copy(k, slot):
        peer = lax.rem(me_dp + k, dp_size)
        return pltpu.make_async_remote_copy(
            src_ref=facts,
            dst_ref=facts_all.at[slot],
            send_sem=fact_send.at[k],
            recv_sem=fact_recv.at[slot],
            device_id=(peer, me_mp),
            device_id_type=MESH,
        )

    each(1, dp_size, lambda k: fact_copy(k, me_dp).start())
    facts_all[me_dp] = facts[...]
    lax.fori_loop(split, CHUNKS, chunk_step, 0)

    sub = lax.broadcasted_iota(jnp.int32, (LANES, LANES), 0)
    for b in range(bands):
        block = slice(b * LANES, (b + 1) * LANES)
        high = peak_rows[block, :].T
        total = total_rows_ref[block, :].T
        moment = moment_rows[block, :].T
        held = target_rows[block, :].T
        peak = jnp.max(high, axis=0, keepdims=True)
        gap = high - peak
        factor = jnp.exp(gap)
        local = targets_v[b : b + 1, :] - base
        inside = (local >= 0) & (local < vocab)
        at_lane = jnp.where(inside, jnp.bitwise_and(local, LANES - 1), -1)
        stats[b : b + 1, :] = peak
        stats[bands + b : bands + b + 1, :] = jnp.sum(factor * total, axis=0, keepdims=True)
        stats[2 * bands + b : 2 * bands + b + 1, :] = jnp.sum(
            factor * (moment + gap * total), axis=0, keepdims=True
        )
        stats[3 * bands + b : 3 * bands + b + 1, :] = jnp.sum(
            jnp.where(sub == at_lane, held, 0.0), axis=0, keepdims=True
        )

    def stat_copy(k, slot):
        peer = lax.rem(me_mp + k, mp_size)
        return pltpu.make_async_remote_copy(
            src_ref=stats,
            dst_ref=gathered.at[slot],
            send_sem=stat_send.at[k],
            recv_sem=stat_recv.at[slot],
            device_id=(me_dp, peer),
            device_id_type=MESH,
        )

    each(1, mp_size, lambda k: stat_copy(k, me_mp).start())
    gathered[me_mp] = stats[...]

    each(1, dp_size, lambda k: fact_copy(k, lax.rem(me_dp + dp_size - k, dp_size)).wait_recv())
    all_reward = facts_all[:, 0:bands, :]
    all_group = facts_all[:, bands : 2 * bands, :]
    all_live = facts_all[:, 2 * bands : 3 * bands, :]

    def whole_sum(values):
        flat = jnp.sum(values, axis=0)
        return jnp.sum(jnp.sum(flat, axis=1, keepdims=True), axis=0, keepdims=True)

    reward_row = rewards_v[...].astype(f32) / reward_unit
    mean_row = jnp.zeros((1, rollouts), f32)
    spread_row = jnp.ones((1, rollouts), f32)
    mean_tok = jnp.zeros((bands, LANES), f32)
    spread_tok = jnp.ones((bands, LANES), f32)
    scale_tok = jnp.zeros((bands, LANES), f32)
    for g in range(groups):
        member = jnp.where(all_group == float(g), 1.0, 0.0).astype(f32)
        mean = whole_sum(member * all_reward) / (GROUP * WIN)
        apart = all_reward - mean[None]
        variance = whole_sum(member * apart * apart) / (GROUP * WIN)
        spread = jnp.maximum(jnp.sqrt(variance), spread_floor)
        scale = (GROUP * WIN) / whole_sum(member * all_live)
        in_row = groups_v[...] == g
        in_tok = group_tok == g
        mean_row = jnp.where(in_row, mean, mean_row)
        spread_row = jnp.where(in_row, spread, spread_row)
        mean_tok = jnp.where(in_tok, mean, mean_tok)
        spread_tok = jnp.where(in_tok, spread, spread_tok)
        scale_tok = jnp.where(in_tok, scale, scale_tok)
    result[3 * bands : 3 * bands + 1, 0:rollouts] = (reward_row - mean_row) / spread_row
    weight = live * ((reward_tok - mean_tok) / spread_tok * scale_tok)
    result[0:bands, :] = weight

    each(1, mp_size, lambda k: stat_copy(k, lax.rem(me_mp + mp_size - k, mp_size)).wait_recv())
    peaks = gathered[:, 0:bands, :]
    peak = jnp.max(peaks, axis=0)
    gap = peaks - peak[None]
    factor = jnp.exp(gap)
    totals = gathered[:, bands : 2 * bands, :]
    total = jnp.sum(factor * totals, axis=0)
    moment = jnp.sum(factor * (gathered[:, 2 * bands : 3 * bands, :] + gap * totals), axis=0)
    target = jnp.sum(gathered[:, 3 * bands : 4 * bands, :], axis=0)
    log_total = jnp.log(total)
    logprob = live * (target - (peak + log_total))
    result[bands : 2 * bands, :] = logprob
    own = jnp.sum(jnp.sum(weight * logprob, axis=1, keepdims=True), axis=0, keepdims=True)
    part[...] = jnp.broadcast_to(own, part.shape)

    def part_copy(k, slot):
        peer = lax.rem(me_dp + k, dp_size)
        return pltpu.make_async_remote_copy(
            src_ref=part,
            dst_ref=parts.at[slot],
            send_sem=part_send.at[k],
            recv_sem=part_recv.at[slot],
            device_id=(peer, me_mp),
            device_id_type=MESH,
        )

    each(1, dp_size, lambda k: part_copy(k, me_dp).start())
    parts[me_dp] = part[...]
    result[2 * bands : 3 * bands, :] = live * (log_total - moment / total)

    each(1, dp_size, lambda k: fact_copy(k, me_dp).wait_send())
    each(1, mp_size, lambda k: stat_copy(k, me_mp).wait_send())
    each(1, dp_size, lambda k: part_copy(k, lax.rem(me_dp + dp_size - k, dp_size)).wait_recv())
    summed = jnp.sum(parts[...], axis=0)[0:1, 0:1]
    result[3 * bands + 1 : 3 * bands + 2, 0:1] = -summed / (groups * GROUP * WIN)
    each(1, dp_size, lambda k: part_copy(k, me_dp).wait_send())


def hand_over(result, advantage, weight, logprob, entropy, objective):
    bands = weight.shape[0]
    weight[...] = result[0:bands, :]
    logprob[...] = result[bands : 2 * bands, :]
    entropy[...] = result[2 * bands : 3 * bands, :]
    advantage[...] = result[3 * bands : 3 * bands + 1, 0 : advantage.shape[1]]
    objective[...] = result[3 * bands + 1 : 3 * bands + 2, 0:1]


def shards(dp_size, mp_size, rewards, group_ids, lengths, token_mask, targets, logits):
    rows, vocab = logits.shape
    rollouts = lengths.shape[0]
    bands = rows // LANES
    f32 = jnp.float32
    anywhere = pl.BlockSpec(memory_space=pl.ANY)
    vmem = pl.BlockSpec(memory_space=pltpu.VMEM)
    result = pl.pallas_call(
        functools.partial(kernel, dp_size, mp_size),
        out_shape=jax.ShapeDtypeStruct((3 * bands + 2, LANES), f32),
        in_specs=[anywhere] * 8,
        out_specs=vmem,
        scratch_shapes=[pltpu.VMEM((rows, vocab), logits.dtype)]
        + [pltpu.SMEM((rollouts,), jnp.int32)] * 3
        + [pltpu.VMEM((1, rollouts), jnp.int32)] * 2
        + [pltpu.VMEM((bands, LANES), jnp.int32)] * 2
        + [pltpu.VMEM((rows, LANES), f32)] * 4
        + [pltpu.VMEM((rows, LANES), jnp.int32)]
        + [
            pltpu.VMEM((4 * bands, LANES), f32),
            pltpu.VMEM((mp_size, 4 * bands, LANES), f32),
            pltpu.VMEM((3 * bands, LANES), f32),
            pltpu.VMEM((dp_size, 3 * bands, LANES), f32),
            pltpu.VMEM((8, LANES), f32),
            pltpu.VMEM((dp_size, 8, LANES), f32),
            pltpu.SemaphoreType.DMA((rows // STEP,)),
            pltpu.SemaphoreType.DMA((7,)),
            pltpu.SemaphoreType.DMA((mp_size,)),
            pltpu.SemaphoreType.DMA((mp_size,)),
            pltpu.SemaphoreType.DMA((dp_size,)),
            pltpu.SemaphoreType.DMA((dp_size,)),
            pltpu.SemaphoreType.DMA((dp_size,)),
            pltpu.SemaphoreType.DMA((dp_size,)),
        ],
        compiler_params=pltpu.CompilerParams(collective_id=0, has_side_effects=True),
    )(
        rewards,
        group_ids,
        lengths,
        rewards.reshape(1, rollouts),
        group_ids.reshape(1, rollouts),
        token_mask.reshape(bands, LANES),
        targets.reshape(bands, LANES),
        logits,
    )
    advantage, weight, logprob, entropy, objective = pl.pallas_call(
        hand_over,
        out_shape=(
            jax.ShapeDtypeStruct((1, rollouts), f32),
            jax.ShapeDtypeStruct((bands, LANES), f32),
            jax.ShapeDtypeStruct((bands, LANES), f32),
            jax.ShapeDtypeStruct((bands, LANES), f32),
            jax.ShapeDtypeStruct((1, 1), f32),
        ),
        in_specs=[vmem],
        out_specs=[vmem] * 5,
    )(result)
    return (
        advantage.reshape(-1),
        weight.reshape(-1),
        logprob.reshape(-1),
        entropy.reshape(-1),
        objective.reshape(()),
    )


def solution(mesh):
    in_specs = (P("dp"), P("dp"), P("dp"), P("dp"), P("dp"), P("dp", "mp"))
    out_specs = (P("dp"), P("dp"), P("dp"), P("dp"), P())
    body = functools.partial(shards, mesh.shape["dp"], mesh.shape["mp"])
    return jax.shard_map(body, mesh=mesh, in_specs=in_specs, out_specs=out_specs, check_vma=False)
```

```python
import functools

import jax
import jax.numpy as jnp
from jax import lax
from jax.experimental import pallas as pl
from jax.experimental.pallas import tpu as pltpu
from jax.sharding import PartitionSpec as P

GROUP = 16
WIN = 64
LANES = 128
STEP = 16
CHUNKS = 8
SUM_ROWS = 16
SUM_TILES = 64
PARTS = 4
AHEAD = 8

spread_floor = 0.25
reward_unit = 1024.0
MESH = pl.DeviceIdType.MESH


def each(first, last, visit):
    if last - first <= 16:
        for k in range(first, last):
            visit(k)
    else:
        lax.fori_loop(first, last, lambda k, carry: (visit(k), carry)[1], 0)


def kernel(
    dp_size,
    mp_size,
    rewards_hbm,
    groups_hbm,
    lengths_hbm,
    rewards_row_hbm,
    groups_row_hbm,
    mask_hbm,
    targets_hbm,
    logits_hbm,
    result,
    block_rows,
    rewards_s,
    groups_s,
    lengths_s,
    rewards_v,
    groups_v,
    mask_v,
    targets_v,
    peak_rows,
    total_rows_ref,
    moment_rows,
    target_rows,
    columns,
    stats,
    gathered,
    facts,
    facts_all,
    part,
    parts,
    load_sem,
    small_sem,
    stat_send,
    stat_recv,
    fact_send,
    fact_recv,
    part_send,
    part_recv,
):
    rows, vocab = logits_hbm.shape
    rollouts = rewards_v.shape[1]
    bands = rows // LANES
    groups = rollouts * dp_size // GROUP
    tiles = vocab // LANES
    me_dp = lax.axis_index("dp")
    me_mp = lax.axis_index("mp")
    f32 = jnp.float32

    def load(i):
        span = pl.ds(pl.multiple_of(i * STEP, STEP), STEP)
        return pltpu.make_async_copy(logits_hbm.at[span, :], block_rows.at[span, :], load_sem.at[i])

    steps = rows // STEP
    for i in range(min(AHEAD, steps)):
        load(i).start()
    small = [
        pltpu.make_async_copy(source, target, small_sem.at[k])
        for k, (source, target) in enumerate(
            (
                (rewards_hbm, rewards_s),
                (groups_hbm, groups_s),
                (lengths_hbm, lengths_s),
                (rewards_row_hbm, rewards_v),
                (groups_row_hbm, groups_v),
                (mask_hbm, mask_v),
                (targets_hbm, targets_v),
            )
        )
    ]
    for copy in small:
        copy.start()

    barrier = pltpu.get_barrier_semaphore()

    def greet_mp(k):
        peer = lax.rem(me_mp + k, mp_size)
        pl.semaphore_signal(barrier, inc=1, device_id=(me_dp, peer), device_id_type=MESH)

    def greet_dp(k):
        peer = lax.rem(me_dp + k, dp_size)
        pl.semaphore_signal(barrier, inc=1, device_id=(peer, me_mp), device_id_type=MESH)

    each(1, mp_size, greet_mp)
    each(1, dp_size, greet_dp)

    for copy in small:
        copy.wait()

    lane = lax.broadcasted_iota(jnp.int32, (bands, LANES), 1)
    band = lax.broadcasted_iota(jnp.int32, (bands, LANES), 0)
    owner = band * (LANES // WIN) + lane // WIN
    position = lax.rem(lane, WIN)
    reward_tok = jnp.zeros((bands, LANES), jnp.int32)
    group_tok = jnp.zeros((bands, LANES), jnp.int32)
    length_tok = jnp.zeros((bands, LANES), jnp.int32)
    for k in range(rollouts):
        here = owner == k
        reward_tok = jnp.where(here, rewards_s[k], reward_tok)
        group_tok = jnp.where(here, groups_s[k], group_tok)
        length_tok = jnp.where(here, lengths_s[k], length_tok)
    live = jnp.where((mask_v[...] > 0) & (position < length_tok), 1.0, 0.0).astype(f32)
    reward_tok = reward_tok.astype(f32) / reward_unit
    facts[0:bands, :] = reward_tok
    facts[bands : 2 * bands, :] = group_tok.astype(f32)
    facts[2 * bands : 3 * bands, :] = live

    base = me_mp * vocab
    for b in range(bands):
        spread_out = jnp.broadcast_to(targets_v[b : b + 1, :], (LANES, LANES))
        columns[b * LANES : (b + 1) * LANES, :] = spread_out.T

    levels = max(tiles - 1, 0).bit_length()

    def survey_step(i, carry):
        load(i).wait()

        @pl.when(i + AHEAD < steps)
        def _():
            load(i + AHEAD).start()

        span = pl.ds(pl.multiple_of(i * STEP, STEP), STEP)
        column = lax.shift_right_arithmetic(columns[span, :] - base, 7)
        bits = [
            jnp.bitwise_and(lax.shift_right_arithmetic(column, k), 1).astype(f32)
            for k in range(levels)
        ]
        bits = [bit.astype(jnp.bfloat16) > 0.5 for bit in bits]

        def survey(first, size):
            if size == 1:
                tile = block_rows[span, first * LANES : (first + 1) * LANES]
                return tile, tile
            half = size // 2
            low = survey(first, half)
            if first + half >= tiles:
                return low
            top = survey(first + half, half)
            chosen = jnp.where(bits[half.bit_length() - 1], top[1], low[1])
            return jnp.maximum(low[0], top[0]), chosen

        high, held = survey(0, 1 << levels)
        target_rows[span, :] = held.astype(f32)
        peak_rows[span, :] = high.astype(f32)
        return carry

    block = min(SUM_TILES, tiles)

    def sum_step(i, carry):
        span = pl.ds(pl.multiple_of(i * SUM_ROWS, SUM_ROWS), SUM_ROWS)
        high = peak_rows[span, :]

        def add_block(q, sums):
            totals, moments = list(sums[:PARTS]), list(sums[PARTS:])
            for j in range(block):
                at = pl.ds(pl.multiple_of((q * block + j) * LANES, LANES), LANES)
                shifted = block_rows[span, at].astype(f32) - high
                weight = jnp.exp(shifted)
                totals[j % PARTS] += weight
                moments[j % PARTS] += weight * shifted
            return (*totals, *moments)

        zero = jnp.zeros((SUM_ROWS, LANES), f32)
        sums = lax.fori_loop(0, tiles // block, add_block, (zero,) * (2 * PARTS))
        total_rows_ref[span, :] = functools.reduce(jnp.add, sums[:PARTS])
        moment_rows[span, :] = functools.reduce(jnp.add, sums[PARTS:])
        return carry

    def chunk_step(c, carry):
        first = c * (steps // CHUNKS)
        lax.fori_loop(first, first + steps // CHUNKS, survey_step, 0)
        low = c * (rows // SUM_ROWS // CHUNKS)
        lax.fori_loop(low, low + rows // SUM_ROWS // CHUNKS, sum_step, 0)
        return carry

    split = CHUNKS // 2
    lax.fori_loop(0, split, chunk_step, 0)
    pl.semaphore_wait(barrier, mp_size + dp_size - 2)

    def fact_copy(k, slot):
        peer = lax.rem(me_dp + k, dp_size)
        return pltpu.make_async_remote_copy(
            src_ref=facts,
            dst_ref=facts_all.at[slot],
            send_sem=fact_send.at[k],
            recv_sem=fact_recv.at[slot],
            device_id=(peer, me_mp),
            device_id_type=MESH,
        )

    each(1, dp_size, lambda k: fact_copy(k, me_dp).start())
    facts_all[me_dp] = facts[...]
    lax.fori_loop(split, CHUNKS, chunk_step, 0)

    sub = lax.broadcasted_iota(jnp.int32, (LANES, LANES), 0)
    for b in range(bands):
        block = slice(b * LANES, (b + 1) * LANES)
        high = peak_rows[block, :].T
        total = total_rows_ref[block, :].T
        moment = moment_rows[block, :].T
        held = target_rows[block, :].T
        peak = jnp.max(high, axis=0, keepdims=True)
        gap = high - peak
        factor = jnp.exp(gap)
        local = targets_v[b : b + 1, :] - base
        inside = (local >= 0) & (local < vocab)
        at_lane = jnp.where(inside, jnp.bitwise_and(local, LANES - 1), -1)
        stats[b : b + 1, :] = peak
        stats[bands + b : bands + b + 1, :] = jnp.sum(factor * total, axis=0, keepdims=True)
        stats[2 * bands + b : 2 * bands + b + 1, :] = jnp.sum(
            factor * (moment + gap * total), axis=0, keepdims=True
        )
        stats[3 * bands + b : 3 * bands + b + 1, :] = jnp.sum(
            jnp.where(sub == at_lane, held, 0.0), axis=0, keepdims=True
        )

    def stat_copy(k, slot):
        peer = lax.rem(me_mp + k, mp_size)
        return pltpu.make_async_remote_copy(
            src_ref=stats,
            dst_ref=gathered.at[slot],
            send_sem=stat_send.at[k],
            recv_sem=stat_recv.at[slot],
            device_id=(me_dp, peer),
            device_id_type=MESH,
        )

    each(1, mp_size, lambda k: stat_copy(k, me_mp).start())
    gathered[me_mp] = stats[...]

    each(1, dp_size, lambda k: fact_copy(k, lax.rem(me_dp + dp_size - k, dp_size)).wait_recv())
    all_reward = facts_all[:, 0:bands, :]
    all_group = facts_all[:, bands : 2 * bands, :]
    all_live = facts_all[:, 2 * bands : 3 * bands, :]

    def whole_sum(values):
        flat = jnp.sum(values, axis=0)
        return jnp.sum(jnp.sum(flat, axis=1, keepdims=True), axis=0, keepdims=True)

    reward_row = rewards_v[...].astype(f32) / reward_unit
    mean_row = jnp.zeros((1, rollouts), f32)
    spread_row = jnp.ones((1, rollouts), f32)
    mean_tok = jnp.zeros((bands, LANES), f32)
    spread_tok = jnp.ones((bands, LANES), f32)
    scale_tok = jnp.zeros((bands, LANES), f32)
    for g in range(groups):
        member = jnp.where(all_group == float(g), 1.0, 0.0).astype(f32)
        mean = whole_sum(member * all_reward) / (GROUP * WIN)
        apart = all_reward - mean[None]
        variance = whole_sum(member * apart * apart) / (GROUP * WIN)
        spread = jnp.maximum(jnp.sqrt(variance), spread_floor)
        scale = (GROUP * WIN) / whole_sum(member * all_live)
        in_row = groups_v[...] == g
        in_tok = group_tok == g
        mean_row = jnp.where(in_row, mean, mean_row)
        spread_row = jnp.where(in_row, spread, spread_row)
        mean_tok = jnp.where(in_tok, mean, mean_tok)
        spread_tok = jnp.where(in_tok, spread, spread_tok)
        scale_tok = jnp.where(in_tok, scale, scale_tok)
    result[3 * bands : 3 * bands + 1, 0:rollouts] = (reward_row - mean_row) / spread_row
    weight = live * ((reward_tok - mean_tok) / spread_tok * scale_tok)
    result[0:bands, :] = weight

    each(1, mp_size, lambda k: stat_copy(k, lax.rem(me_mp + mp_size - k, mp_size)).wait_recv())
    peaks = gathered[:, 0:bands, :]
    peak = jnp.max(peaks, axis=0)
    gap = peaks - peak[None]
    factor = jnp.exp(gap)
    totals = gathered[:, bands : 2 * bands, :]
    total = jnp.sum(factor * totals, axis=0)
    moment = jnp.sum(factor * (gathered[:, 2 * bands : 3 * bands, :] + gap * totals), axis=0)
    target = jnp.sum(gathered[:, 3 * bands : 4 * bands, :], axis=0)
    log_total = jnp.log(total)
    logprob = live * (target - (peak + log_total))
    result[bands : 2 * bands, :] = logprob
    own = jnp.sum(jnp.sum(weight * logprob, axis=1, keepdims=True), axis=0, keepdims=True)
    part[...] = jnp.broadcast_to(own, part.shape)

    def part_copy(k, slot):
        peer = lax.rem(me_dp + k, dp_size)
        return pltpu.make_async_remote_copy(
            src_ref=part,
            dst_ref=parts.at[slot],
            send_sem=part_send.at[k],
            recv_sem=part_recv.at[slot],
            device_id=(peer, me_mp),
            device_id_type=MESH,
        )

    each(1, dp_size, lambda k: part_copy(k, me_dp).start())
    parts[me_dp] = part[...]
    result[2 * bands : 3 * bands, :] = live * (log_total - moment / total)

    each(1, dp_size, lambda k: fact_copy(k, me_dp).wait_send())
    each(1, mp_size, lambda k: stat_copy(k, me_mp).wait_send())
    each(1, dp_size, lambda k: part_copy(k, lax.rem(me_dp + dp_size - k, dp_size)).wait_recv())
    summed = jnp.sum(parts[...], axis=0)[0:1, 0:1]
    result[3 * bands + 1 : 3 * bands + 2, 0:1] = -summed / (groups * GROUP * WIN)
    each(1, dp_size, lambda k: part_copy(k, me_dp).wait_send())


def hand_over(result, advantage, weight, logprob, entropy, objective):
    bands = weight.shape[0]
    weight[...] = result[0:bands, :]
    logprob[...] = result[bands : 2 * bands, :]
    entropy[...] = result[2 * bands : 3 * bands, :]
    advantage[...] = result[3 * bands : 3 * bands + 1, 0 : advantage.shape[1]]
    objective[...] = result[3 * bands + 1 : 3 * bands + 2, 0:1]


def shards(dp_size, mp_size, rewards, group_ids, lengths, token_mask, targets, logits):
    rows, vocab = logits.shape
    rollouts = lengths.shape[0]
    bands = rows // LANES
    f32 = jnp.float32
    anywhere = pl.BlockSpec(memory_space=pl.ANY)
    vmem = pl.BlockSpec(memory_space=pltpu.VMEM)
    result = pl.pallas_call(
        functools.partial(kernel, dp_size, mp_size),
        out_shape=jax.ShapeDtypeStruct((3 * bands + 2, LANES), f32),
        in_specs=[anywhere] * 8,
        out_specs=vmem,
        scratch_shapes=[pltpu.VMEM((rows, vocab), logits.dtype)]
        + [pltpu.SMEM((rollouts,), jnp.int32)] * 3
        + [pltpu.VMEM((1, rollouts), jnp.int32)] * 2
        + [pltpu.VMEM((bands, LANES), jnp.int32)] * 2
        + [pltpu.VMEM((rows, LANES), f32)] * 4
        + [pltpu.VMEM((rows, LANES), jnp.int32)]
        + [
            pltpu.VMEM((4 * bands, LANES), f32),
            pltpu.VMEM((mp_size, 4 * bands, LANES), f32),
            pltpu.VMEM((3 * bands, LANES), f32),
            pltpu.VMEM((dp_size, 3 * bands, LANES), f32),
            pltpu.VMEM((8, LANES), f32),
            pltpu.VMEM((dp_size, 8, LANES), f32),
            pltpu.SemaphoreType.DMA((rows // STEP,)),
            pltpu.SemaphoreType.DMA((7,)),
            pltpu.SemaphoreType.DMA((mp_size,)),
            pltpu.SemaphoreType.DMA((mp_size,)),
            pltpu.SemaphoreType.DMA((dp_size,)),
            pltpu.SemaphoreType.DMA((dp_size,)),
            pltpu.SemaphoreType.DMA((dp_size,)),
            pltpu.SemaphoreType.DMA((dp_size,)),
        ],
        compiler_params=pltpu.CompilerParams(collective_id=0, has_side_effects=True),
    )(
        rewards,
        group_ids,
        lengths,
        rewards.reshape(1, rollouts),
        group_ids.reshape(1, rollouts),
        token_mask.reshape(bands, LANES),
        targets.reshape(bands, LANES),
        logits,
    )
    advantage, weight, logprob, entropy, objective = pl.pallas_call(
        hand_over,
        out_shape=(
            jax.ShapeDtypeStruct((1, rollouts), f32),
            jax.ShapeDtypeStruct((bands, LANES), f32),
            jax.ShapeDtypeStruct((bands, LANES), f32),
            jax.ShapeDtypeStruct((bands, LANES), f32),
            jax.ShapeDtypeStruct((1, 1), f32),
        ),
        in_specs=[vmem],
        out_specs=[vmem] * 5,
    )(result)
    return (
        advantage.reshape(-1),
        weight.reshape(-1),
        logprob.reshape(-1),
        entropy.reshape(-1),
        objective.reshape(()),
    )


def solution(mesh):
    in_specs = (P("dp"), P("dp"), P("dp"), P("dp"), P("dp"), P("dp", "mp"))
    out_specs = (P("dp"), P("dp"), P("dp"), P("dp"), P())
    body = functools.partial(shards, mesh.shape["dp"], mesh.shape["mp"])
    return jax.shard_map(body, mesh=mesh, in_specs=in_specs, out_specs=out_specs, check_vma=False)
```
